32 devices in a mesh: seq: 8 (over z, y), head: 4 (over x, core).
Axes of the slice: x: 2, y: 2, z: 4, core: 2. Of those that a mesh axis runs over, the one named last changes fastest.
Arguments:
- queries: bfloat16 [1024, 4096], P('seq', 'head'), may hold values from -40 to 40
- keys: bfloat16 [1024, 512], P(('seq', 'head')), may hold values from -40 to 40
- values: bfloat16 [1024, 512], P(('seq', 'head')), may hold values from -6 to 6
- block_order: int32 [8], replicated, may hold values from 0 to 7, each once
Outputs:
- attended: bfloat16 [1024, 4096], P('seq', 'head')
The draws below stay inside these ranges and needn't reach their ends.
All inputs are finite; a program needn't handle non-finite values.
Results may differ from the reference program's by a relative error of at most 0.0055.
Values may be sent and summed in bfloat16 or wider, within the bound.
A program may use at most 64 MiB of HBM per device.

```python
import math
import jax
import jax.numpy as jnp
from jax import lax

HD = 128
QH = 32
KVH = 4
TOK_DEV = 128
GROUP = 8
TOKENS = 1024
N_SEQ = 8


def joint_draw(key):
    base = jax.random.fold_in(key, 11)
    key_query, key_key = jax.random.split(base, 2)
    query_part = jax.random.normal(key_query, (TOKENS, KVH, GROUP, HD), jnp.float32)
    key_part = jax.random.normal(key_key, (TOKENS, KVH, HD), jnp.float32)
    query_part = jnp.clip(query_part, -40.0, 40.0)
    key_part = jnp.clip(key_part, -40.0, 40.0)
    return (query_part.reshape(TOKENS, QH * HD), key_part.reshape(TOKENS, KVH * HD))


def draw_queries(key, part):
    return joint_draw(key)[0].astype(jnp.bfloat16)


def draw_keys(key, part):
    return joint_draw(key)[1].astype(jnp.bfloat16)


def levels(own_key, extent, shards, low, high):
    def one(axis_at, shards_of):
        heights = jax.random.uniform(jax.random.fold_in(jax.random.fold_in(own_key, 6), axis_at), (shards_of,), jnp.float32, low / len(shards), high / len(shards))
        return jnp.repeat(jnp.exp(heights), extent[axis_at] // shards_of).reshape((-1,) + (1,) * (len(extent) - axis_at - 1))

    loudness = one(*shards[0])
    for cut in shards[1:]:
        loudness = loudness * one(*cut)
    return loudness


def gaussian(own_key, extent, width, reach, shards=(), held_as=jnp.bfloat16):
    factor_of = levels(own_key, extent, shards, -0.22, 0.18) if shards else 1.0
    values = jax.random.normal(own_key, extent, jnp.float32) * width * factor_of
    return jnp.minimum(jnp.maximum(values, -reach), reach).astype(held_as)


def setup_inputs(seed: int = 0) -> dict:
    seeds = jax.random.split(jax.random.key(seed), 5)
    return {
        "queries": draw_queries(jax.random.fold_in(seeds[4], 71), 0),
        "keys": draw_keys(jax.random.fold_in(seeds[4], 71), 0),
        "values": gaussian(seeds[2], (TOKENS, KVH * HD), 1.0, 6.0, ((0, 32),)),
        "block_order": jax.random.permutation(seeds[3], N_SEQ).astype(jnp.int32),
    }


def reference(queries, keys, values, block_order):
    position = (block_order[:, None] * TOK_DEV + jnp.arange(TOK_DEV, dtype=jnp.int32)[None, :]).reshape(-1).astype(jnp.int32)
    query_heads = queries.reshape(TOKENS, KVH, GROUP, HD)
    key_heads = keys.reshape(TOKENS, KVH, HD)
    value_heads = values.reshape(TOKENS, KVH, HD)
    row_block = math.gcd(TOKENS, 512)
    factor = 1.0 / math.sqrt(HD)

    def per_head(head_index):
        key_cols = lax.dynamic_index_in_dim(key_heads, head_index, 1, keepdims=False).astype(jnp.float32)
        value_cols = lax.dynamic_index_in_dim(value_heads, head_index, 1, keepdims=False).astype(jnp.float32)
        query_cols = lax.dynamic_index_in_dim(query_heads, head_index, 1, keepdims=False)

        def per_block(block_index):
            start = (block_index * row_block).astype(jnp.int32)
            query_rows = lax.dynamic_slice_in_dim(query_cols, start, row_block, 0).astype(jnp.float32)
            query_pos = lax.dynamic_slice_in_dim(position, start, row_block, 0)
            scores = jnp.einsum('qgd,kd->gqk', query_rows, key_cols) * factor
            visible = (query_pos[:, None] >= position[None, :])[None]
            scores = jnp.where(visible, scores, -1e+30)
            highest = lax.optimization_barrier(jnp.max(scores, axis=-1, keepdims=True))
            weights = jnp.where(visible, jnp.exp(scores - highest), 0.0)
            totals = lax.optimization_barrier(jnp.sum(weights, axis=-1))
            rounded = lax.optimization_barrier(weights.astype(jnp.bfloat16)).astype(jnp.float32)
            numerator = jnp.einsum('gqk,kd->qgd', rounded, value_cols)
            return numerator / jnp.transpose(totals)[:, :, None]
        result = lax.map(per_block, jnp.arange(TOKENS // row_block, dtype=jnp.int32))
        return result.reshape(TOKENS, GROUP, HD)
    every = lax.map(per_head, jnp.arange(KVH, dtype=jnp.int32))
    return jnp.transpose(every, (1, 0, 2, 3)).reshape(TOKENS, QH * HD).astype(jnp.bfloat16)
```

```python
import functools
import math

import jax
import jax.numpy as jnp
from jax import lax
from jax.experimental import pallas as pl
from jax.experimental.pallas import tpu as pltpu
from jax.sharding import PartitionSpec as P

HD = 128
NEG = -1e30
MESH = pl.DeviceIdType.MESH


def kernel(
    outer, inner, heads,
    order, q_hbm, k_hbm, v_hbm, out_ref,
    q_ref, k_ref, v_ref, kz, vz, kd, vd, acc, high, total,
    load_sem, zsend, zrecv, psend, precv,
):
    rows, _ = k_ref.shape
    block = q_ref.shape[0]
    width = kd.shape[-1]
    q_heads = q_ref.shape[1] // HD
    seq, head = lax.axis_index("seq"), lax.axis_index("head")
    o, j = seq // inner, lax.rem(seq, inner)
    power = outer & (outer - 1) == 0

    def source(k):
        return jnp.bitwise_xor(o, k) if power else lax.rem(o - k + outer, outer)

    def target(k):
        return jnp.bitwise_xor(o, k) if power else lax.rem(o + k, outer)

    loads = [
        pltpu.make_async_copy(src, dst, load_sem.at[i])
        for i, (src, dst) in enumerate(((k_hbm, k_ref), (v_hbm, v_ref), (q_hbm, q_ref)))
    ]
    for load in loads:
        load.start()

    group = [(dj, dh) for dj in range(inner) for dh in range(heads)]

    def member(dj, dh):
        return lax.rem(j + dj, inner), lax.rem(head + dh, heads)

    barrier = pltpu.get_barrier_semaphore()
    for dj, dh in group[1:]:
        j2, h2 = member(dj, dh)
        pl.semaphore_signal(barrier, inc=1, device_id=(o * inner + j2, h2), device_id_type=MESH)

    def greet(k, c):
        pl.semaphore_signal(
            barrier, inc=1, device_id=(target(k) * inner + j, head), device_id_type=MESH
        )
        return c

    def steps(first, last, body):
        if last - first <= 8:
            for k in range(first, last):
                body(k, 0)
        else:
            lax.fori_loop(first, last, body, 0)

    steps(1, outer, greet)
    pl.semaphore_wait(barrier, len(group) - 1 + outer - 1)
    loads[0].wait()
    loads[1].wait()

    def zcopy(k, which):
        own, far = ((k_ref, kz), (v_ref, vz))[which]
        return pltpu.make_async_remote_copy(
            src_ref=own,
            dst_ref=far.at[k - 1],
            send_sem=zsend.at[which],
            recv_sem=zrecv.at[k, which],
            device_id=(target(k) * inner + j, head),
            device_id_type=MESH,
        )

    def scatter(piece, k, which):
        dst = (kd, vd)[which]
        place = pl.ds(pl.multiple_of(j * block + head * rows, rows), rows)
        for dj, dh in group:
            j2, h2 = member(dj, dh)
            src = piece.at[:, pl.ds(pl.multiple_of(h2 * width, width), width)]
            if dj == 0 and dh == 0:
                pltpu.make_async_copy(src, dst.at[k, place], load_sem.at[3 + which]).start()
            else:
                pltpu.make_async_remote_copy(
                    src_ref=src,
                    dst_ref=dst.at[k, place],
                    send_sem=psend.at[k, which],
                    recv_sem=precv.at[k, which],
                    device_id=(o * inner + j2, h2),
                    device_id_type=MESH,
                ).start()
        src = piece.at[:, pl.ds(pl.multiple_of(head * width, width), width)]
        pltpu.make_async_copy(src, dst.at[k, place], load_sem.at[3 + which]).wait()

    others = pl.ds(0, (len(group) - 1) * rows)

    def landed(k, which):
        dst = (kd, vd)[which].at[k, others]
        pltpu.make_async_copy(dst, dst, precv.at[k, which]).wait()

    def relay(k, c=0):
        for which in range(2):
            zcopy(k, which).wait_recv()
            scatter((kz, vz)[which].at[k - 1], k, which)
        return c

    mine = order[seq]
    factor = math.log2(math.e) / math.sqrt(HD)
    per = 2 if q_heads % 2 == 0 else 1
    lanes = per * block
    count = inner * block

    def absorb(k, first):
        src = source(k) * inner
        row = lax.broadcasted_iota(jnp.int32, (count, lanes), 0)
        col = lax.broadcasted_iota(jnp.int32, (count, lanes), 1)
        start = jnp.full((count, lanes), order[src], jnp.int32) * block
        for jj in range(1, inner):
            start = jnp.where(row >= jj * block, order[src + jj] * block - jj * block, start)
        visible = mine * block + lax.rem(col, block) >= start + row
        landed(k, 0)
        key = kd[k]
        for c in range(q_heads // per):
            q = jnp.concatenate(
                [q_ref[:, (c * per + i) * HD : (c * per + i + 1) * HD] for i in range(per)], axis=0
            )
            s = lax.dot_general(
                key, q, (((1,), (1,)), ((), ())), preferred_element_type=jnp.float32
            )
            s = jnp.where(visible, s * factor, NEG)
            at = slice(c * lanes, (c + 1) * lanes)
            top = jnp.max(s, axis=0, keepdims=True)
            if not first:
                old = high[:, at]
                top = jnp.maximum(old, top)
            p = jnp.exp2(s - top)
            high[:, at] = top
            t = jnp.sum(p, axis=0, keepdims=True)
            if c == 0:
                landed(k, 1)
                value = vd[k]
            pv = lax.dot_general(
                value,
                p.astype(jnp.bfloat16),
                (((0,), (0,)), ((), ())),
                preferred_element_type=jnp.float32,
            )
            if first:
                total[:, at] = t
                acc[:, at] = pv
            else:
                scale = jnp.exp2(old - top)
                total[:, at] = total[:, at] * scale + t
                acc[:, at] = acc[:, at] * scale + pv

    for which in range(2):
        steps(1, outer, lambda k, c, which=which: (zcopy(k, which).start(), c)[1])
        scatter((k_ref, v_ref)[which], 0, which)
    loads[2].wait()
    if outer > 1:
        relay(1)
    absorb(0, True)

    def later(k, c):
        relay(k + 1)
        absorb(k, False)
        return c

    steps(1, outer - 1, later)
    if outer > 1:
        absorb(outer - 1, False)

    for g in range(q_heads):
        at = slice(g * HD, (g + 1) * HD)
        lane = slice(g * block, (g + 1) * block)
        part = acc[:, lane] / total[:, lane]
        out_ref[:, at] = part.T.astype(out_ref.dtype)

    if outer > 1:
        for which in range(2):
            sent = (kz, vz)[which]
            pltpu.make_async_copy(sent, sent, zsend.at[which]).wait()

    def drain(k, c):
        for which in range(2):
            dst = (kd, vd)[which].at[k, others]
            pltpu.make_async_copy(dst, dst, psend.at[k, which]).wait()
        return c

    steps(0, outer, drain)


def local(devices, heads, queries, keys, values, block_order):
    inner = 2 if devices % 2 == 0 else 1
    outer = devices // inner
    rows, cols = keys.shape
    block, q_cols = queries.shape
    width = cols // heads
    assert width == HD and rows * heads == block
    bf16, f32 = jnp.bfloat16, jnp.float32
    far = max(outer - 1, 1)
    return pl.pallas_call(
        functools.partial(kernel, outer, inner, heads),
        out_shape=jax.ShapeDtypeStruct((block, q_cols), queries.dtype),
        in_specs=[pl.BlockSpec(memory_space=pltpu.SMEM)]
        + [pl.BlockSpec(memory_space=pl.ANY)] * 3,
        out_specs=pl.BlockSpec(memory_space=pltpu.VMEM),
        scratch_shapes=[
            pltpu.VMEM((block, q_cols), bf16),
            pltpu.VMEM((rows, cols), bf16),
            pltpu.VMEM((rows, cols), bf16),
            pltpu.VMEM((far, rows, cols), bf16),
            pltpu.VMEM((far, rows, cols), bf16),
            pltpu.VMEM((outer, inner * block, width), bf16),
            pltpu.VMEM((outer, inner * block, width), bf16),
            pltpu.VMEM((HD, q_cols // HD * block), f32),
            pltpu.VMEM((1, q_cols // HD * block), f32),
            pltpu.VMEM((1, q_cols // HD * block), f32),
            pltpu.SemaphoreType.DMA((5,)),
            pltpu.SemaphoreType.DMA((2,)),
            pltpu.SemaphoreType.DMA((outer, 2)),
            pltpu.SemaphoreType.DMA((outer, 2)),
            pltpu.SemaphoreType.DMA((outer, 2)),
        ],
        compiler_params=pltpu.CompilerParams(
            collective_id=0, has_side_effects=True, vmem_limit_bytes=48 * 1024 * 1024
        ),
    )(block_order, queries, keys, values)


def solution(mesh):
    placed = (P("seq", "head"), P(("seq", "head"), None), P(("seq", "head"), None), P())
    return jax.shard_map(
        functools.partial(local, mesh.shape["seq"], mesh.shape["head"]),
        mesh=mesh, in_specs=placed, out_specs=P("seq", "head"), check_vma=False,
    )
```

```python
import functools
import math

import jax
import jax.numpy as jnp
from jax import lax
from jax.experimental import pallas as pl
from jax.experimental.pallas import tpu as pltpu
from jax.sharding import PartitionSpec as P

HD = 128
NEG = -1e30
MESH = pl.DeviceIdType.MESH


def kernel(
    outer, inner, heads,
    order, q_hbm, k_hbm, v_hbm, acc, total,
    q_ref, k_ref, v_ref, kz, vz, kd, vd, high,
    load_sem, zsend, zrecv, psend, precv,
):
    rows, _ = k_ref.shape
    block = q_ref.shape[0]
    width = kd.shape[-1]
    q_heads = q_ref.shape[1] // HD
    seq, head = lax.axis_index("seq"), lax.axis_index("head")
    o, j = seq // inner, lax.rem(seq, inner)
    power = outer & (outer - 1) == 0

    def source(k):
        return jnp.bitwise_xor(o, k) if power else lax.rem(o - k + outer, outer)

    def target(k):
        return jnp.bitwise_xor(o, k) if power else lax.rem(o + k, outer)

    loads = [
        pltpu.make_async_copy(src, dst, load_sem.at[i])
        for i, (src, dst) in enumerate(((k_hbm, k_ref), (v_hbm, v_ref), (q_hbm, q_ref)))
    ]
    for load in loads:
        load.start()

    group = [(dj, dh) for dj in range(inner) for dh in range(heads)]

    def member(dj, dh):
        return lax.rem(j + dj, inner), lax.rem(head + dh, heads)

    barrier = pltpu.get_barrier_semaphore()
    for dj, dh in group[1:]:
        j2, h2 = member(dj, dh)
        pl.semaphore_signal(barrier, inc=1, device_id=(o * inner + j2, h2), device_id_type=MESH)

    def greet(k, c):
        pl.semaphore_signal(
            barrier, inc=1, device_id=(target(k) * inner + j, head), device_id_type=MESH
        )
        return c

    def steps(first, last, body):
        if last - first <= 8:
            for k in range(first, last):
                body(k, 0)
        else:
            lax.fori_loop(first, last, body, 0)

    steps(1, outer, greet)
    pl.semaphore_wait(barrier, len(group) - 1 + outer - 1)
    loads[0].wait()
    loads[1].wait()

    def zcopy(k, which):
        own, far = ((k_ref, kz), (v_ref, vz))[which]
        return pltpu.make_async_remote_copy(
            src_ref=own,
            dst_ref=far.at[k - 1],
            send_sem=zsend.at[which],
            recv_sem=zrecv.at[k, which],
            device_id=(target(k) * inner + j, head),
            device_id_type=MESH,
        )

    def scatter(piece, k, which):
        dst = (kd, vd)[which]
        place = pl.ds(pl.multiple_of(j * block + head * rows, rows), rows)
        for dj, dh in group:
            j2, h2 = member(dj, dh)
            src = piece.at[:, pl.ds(pl.multiple_of(h2 * width, width), width)]
            if dj == 0 and dh == 0:
                pltpu.make_async_copy(src, dst.at[k, place], load_sem.at[3 + which]).start()
            else:
                pltpu.make_async_remote_copy(
                    src_ref=src,
                    dst_ref=dst.at[k, place],
                    send_sem=psend.at[k, which],
                    recv_sem=precv.at[k, which],
                    device_id=(o * inner + j2, h2),
                    device_id_type=MESH,
                ).start()
        src = piece.at[:, pl.ds(pl.multiple_of(head * width, width), width)]
        pltpu.make_async_copy(src, dst.at[k, place], load_sem.at[3 + which]).wait()

    others = pl.ds(0, (len(group) - 1) * rows)

    def landed(k, which):
        dst = (kd, vd)[which].at[k, others]
        pltpu.make_async_copy(dst, dst, precv.at[k, which]).wait()

    def relay(k, c=0):
        for which in range(2):
            zcopy(k, which).wait_recv()
            scatter((kz, vz)[which].at[k - 1], k, which)
        return c

    mine = order[seq]
    factor = math.log2(math.e) / math.sqrt(HD)
    per = 2 if q_heads % 2 == 0 else 1
    lanes = per * block
    count = inner * block

    def absorb(k, first):
        src = source(k) * inner
        row = lax.broadcasted_iota(jnp.int32, (count, lanes), 0)
        col = lax.broadcasted_iota(jnp.int32, (count, lanes), 1)
        start = jnp.full((count, lanes), order[src], jnp.int32) * block
        for jj in range(1, inner):
            start = jnp.where(row >= jj * block, order[src + jj] * block - jj * block, start)
        visible = mine * block + lax.rem(col, block) >= start + row
        landed(k, 0)
        key = kd[k]
        for c in range(q_heads // per):
            q = jnp.concatenate(
                [q_ref[:, (c * per + i) * HD : (c * per + i + 1) * HD] for i in range(per)], axis=0
            )
            s = lax.dot_general(
                key, q, (((1,), (1,)), ((), ())), preferred_element_type=jnp.float32
            )
            s = jnp.where(visible, s * factor, NEG)
            at = slice(c * lanes, (c + 1) * lanes)
            top = jnp.max(s, axis=0, keepdims=True)
            if not first:
                old = high[:, at]
                top = jnp.maximum(old, top)
            p = jnp.exp2(s - top)
            high[:, at] = top
            t = jnp.sum(p, axis=0, keepdims=True)
            if c == 0:
                landed(k, 1)
                value = vd[k]
            pv = lax.dot_general(
                value,
                p.astype(jnp.bfloat16),
                (((0,), (0,)), ((), ())),
                preferred_element_type=jnp.float32,
            )
            if first:
                total[:, at] = t
                acc[:, at] = pv
            else:
                scale = jnp.exp2(old - top)
                total[:, at] = total[:, at] * scale + t
                acc[:, at] = acc[:, at] * scale + pv

    for which in range(2):
        steps(1, outer, lambda k, c, which=which: (zcopy(k, which).start(), c)[1])
        scatter((k_ref, v_ref)[which], 0, which)
    loads[2].wait()
    if outer > 1:
        relay(1)
    absorb(0, True)

    def later(k, c):
        relay(k + 1)
        absorb(k, False)
        return c

    steps(1, outer - 1, later)
    if outer > 1:
        absorb(outer - 1, False)

    if outer > 1:
        for which in range(2):
            sent = (kz, vz)[which]
            pltpu.make_async_copy(sent, sent, zsend.at[which]).wait()

    def drain(k, c):
        for which in range(2):
            dst = (kd, vd)[which].at[k, others]
            pltpu.make_async_copy(dst, dst, psend.at[k, which]).wait()
        return c

    steps(0, outer, drain)


def finish(acc, total, out_ref):
    block, q_cols = out_ref.shape
    for g in range(q_cols // HD):
        lane = slice(g * block, (g + 1) * block)
        part = acc[:, lane] / total[:, lane]
        out_ref[:, g * HD : (g + 1) * HD] = part.T.astype(out_ref.dtype)


def local(devices, heads, queries, keys, values, block_order):
    inner = 2 if devices % 2 == 0 else 1
    outer = devices // inner
    rows, cols = keys.shape
    block, q_cols = queries.shape
    width = cols // heads
    assert width == HD and rows * heads == block
    bf16, f32 = jnp.bfloat16, jnp.float32
    far = max(outer - 1, 1)
    lanes = q_cols // HD * block
    acc, total = pl.pallas_call(
        functools.partial(kernel, outer, inner, heads),
        out_shape=(
            pltpu.VMEM((HD, lanes), f32),
            pltpu.VMEM((1, lanes), f32),
        ),
        in_specs=[pl.BlockSpec(memory_space=pltpu.SMEM)]
        + [pl.BlockSpec(memory_space=pltpu.HBM)] * 3,
        out_specs=[pl.BlockSpec(memory_space=pltpu.VMEM)] * 2,
        scratch_shapes=[
            pltpu.VMEM((block, q_cols), bf16),
            pltpu.VMEM((rows, cols), bf16),
            pltpu.VMEM((rows, cols), bf16),
            pltpu.VMEM((far, rows, cols), bf16),
            pltpu.VMEM((far, rows, cols), bf16),
            pltpu.VMEM((outer, inner * block, width), bf16),
            pltpu.VMEM((outer, inner * block, width), bf16),
            pltpu.VMEM((1, lanes), f32),
            pltpu.SemaphoreType.DMA((5,)),
            pltpu.SemaphoreType.DMA((2,)),
            pltpu.SemaphoreType.DMA((outer, 2)),
            pltpu.SemaphoreType.DMA((outer, 2)),
            pltpu.SemaphoreType.DMA((outer, 2)),
        ],
        compiler_params=pltpu.CompilerParams(
            collective_id=0, has_side_effects=True, vmem_limit_bytes=67043328 - 600 * 1024
        ),
    )(block_order, queries, keys, values)
    return pl.pallas_call(
        finish,
        out_shape=jax.ShapeDtypeStruct((block, q_cols), queries.dtype),
        in_specs=[pl.BlockSpec(memory_space=pltpu.VMEM)] * 2,
        out_specs=pl.BlockSpec(memory_space=pltpu.VMEM),
        compiler_params=pltpu.CompilerParams(vmem_limit_bytes=8 * 1024 * 1024),
    )(acc, total)


def solution(mesh):
    placed = (P("seq", "head"), P(("seq", "head"), None), P(("seq", "head"), None), P())
    return jax.shard_map(
        functools.partial(local, mesh.shape["seq"], mesh.shape["head"]),
        mesh=mesh, in_specs=placed, out_specs=P("seq", "head"), check_vma=False,
    )
```

```python
import functools
import math

import jax
import jax.numpy as jnp
from jax import lax
from jax.experimental import pallas as pl
from jax.experimental.pallas import tpu as pltpu
from jax.sharding import PartitionSpec as P

HD = 128
NEG = -1e30
MESH = pl.DeviceIdType.MESH


def kernel(
    outer, inner, heads,
    order, q_hbm, k_hbm, v_hbm, acc, total,
    q_ref, k_ref, v_ref, kz, vz, kd, vd, high,
    load_sem, own_sem, zsend, zrecv, psend, precv,
):
    rows, _ = k_ref.shape
    block = q_ref.shape[0]
    width = kd.shape[-1]
    q_heads = q_ref.shape[1] // HD
    seq, head = lax.axis_index("seq"), lax.axis_index("head")
    o, j = seq // inner, lax.rem(seq, inner)
    power = outer & (outer - 1) == 0

    bits = [1 << i for i in range(outer.bit_length() - 1)] if power else range(1, outer)

    def source(k):
        return jnp.bitwise_xor(o, k) if power else lax.rem(o - k + outer, outer)

    def target(k):
        return jnp.bitwise_xor(o, k) if power else lax.rem(o + k, outer)

    loads = [
        pltpu.make_async_copy(src, dst, load_sem.at[i])
        for i, (src, dst) in enumerate(((k_hbm, k_ref), (v_hbm, v_ref), (q_hbm, q_ref)))
    ]
    for load in loads:
        load.start()

    group = [(dj, dh) for dj in range(inner) for dh in range(heads)]

    def member(dj, dh):
        return lax.rem(j + dj, inner), lax.rem(head + dh, heads)

    barrier = pltpu.get_barrier_semaphore()
    for dj, dh in group[1:]:
        j2, h2 = member(dj, dh)
        pl.semaphore_signal(barrier, inc=1, device_id=(o * inner + j2, h2), device_id_type=MESH)

    for k in bits:
        pl.semaphore_signal(
            barrier, inc=1, device_id=(target(k) * inner + j, head), device_id_type=MESH
        )

    def steps(first, last, body):
        if last - first <= 8:
            for k in range(first, last):
                body(k, 0)
        else:
            lax.fori_loop(first, last, body, 0)

    pl.semaphore_wait(barrier, len(group) - 1 + len(bits))
    loads[0].wait()
    loads[1].wait()

    def zcopy(piece, k, bit, which):
        return pltpu.make_async_remote_copy(
            src_ref=piece,
            dst_ref=(kz, vz)[which].at[k - 1],
            send_sem=zsend.at[which],
            recv_sem=zrecv.at[k, which],
            device_id=(target(bit) * inner + j, head),
            device_id_type=MESH,
        )

    def forward(piece, k, which):
        for bit in bits:
            if isinstance(k, int):
                if bit < k & -k:
                    zcopy(piece, k + bit, bit, which).start()
            else:

                @pl.when(bit < (k & -k))
                def _(bit=bit):
                    zcopy(piece, k + bit, bit, which).start()

    def scatter(piece, k, which):
        dst = (kd, vd)[which]
        place = pl.ds(pl.multiple_of(j * block + head * rows, rows), rows)
        for dj, dh in group[::-1]:
            j2, h2 = member(dj, dh)
            src = piece.at[:, pl.ds(pl.multiple_of(h2 * width, width), width)]
            if dj == 0 and dh == 0:
                pltpu.make_async_copy(src, dst.at[k, place], own_sem.at[k, which]).start()
            else:
                pltpu.make_async_remote_copy(
                    src_ref=src,
                    dst_ref=dst.at[k, place],
                    send_sem=psend.at[k, which],
                    recv_sem=precv.at[k, which],
                    device_id=(o * inner + j2, h2),
                    device_id_type=MESH,
                ).start()

    others = pl.ds(0, (len(group) - 1) * rows)

    def landed(k, which):
        dst = (kd, vd)[which].at[k, others]
        pltpu.make_async_copy(dst, dst, precv.at[k, which]).wait()
        dst = (kd, vd)[which].at[k, pl.ds(0, rows)]
        pltpu.make_async_copy(dst, dst, own_sem.at[k, which]).wait()

    def relay(k, c=0):
        for which in range(2):
            piece = (kz, vz)[which].at[k - 1]
            zcopy(piece, k, bits[0], which).wait_recv()
            if power:
                forward(piece, k, which)
            scatter(piece, k, which)
        return c

    mine = order[seq]
    factor = math.log2(math.e) / math.sqrt(HD)
    per = 2 if q_heads % 2 == 0 else 1
    lanes = per * block
    count = inner * block

    def absorb(k, first):
        src = source(k) * inner
        row = lax.broadcasted_iota(jnp.int32, (count, lanes), 0)
        col = lax.broadcasted_iota(jnp.int32, (count, lanes), 1)
        start = jnp.full((count, lanes), order[src], jnp.int32) * block
        for jj in range(1, inner):
            start = jnp.where(row >= jj * block, order[src + jj] * block - jj * block, start)
        visible = mine * block + lax.rem(col, block) >= start + row
        landed(k, 0)
        key = kd[k]
        for c in range(q_heads // per):
            q = jnp.concatenate(
                [q_ref[:, (c * per + i) * HD : (c * per + i + 1) * HD] for i in range(per)], axis=0
            )
            s = lax.dot_general(
                key, q, (((1,), (1,)), ((), ())), preferred_element_type=jnp.float32
            )
            s = jnp.where(visible, s * factor, NEG)
            at = slice(c * lanes, (c + 1) * lanes)
            top = jnp.max(s, axis=0, keepdims=True)
            if not first:
                old = high[:, at]
                top = jnp.maximum(old, top)
            p = jnp.exp2(s - top)
            high[:, at] = top
            t = jnp.sum(p, axis=0, keepdims=True)
            if c == 0:
                landed(k, 1)
                value = vd[k]
            pv = lax.dot_general(
                value,
                p.astype(jnp.bfloat16),
                (((0,), (0,)), ((), ())),
                preferred_element_type=jnp.float32,
            )
            if first:
                total[:, at] = t
                acc[:, at] = pv
            else:
                scale = jnp.exp2(old - top)
                total[:, at] = total[:, at] * scale + t
                acc[:, at] = acc[:, at] * scale + pv

    for bit in bits[::-1]:
        for which in range(2):
            zcopy((k_ref, v_ref)[which], bit, bit, which).start()
    for which in range(2):
        scatter((k_ref, v_ref)[which], 0, which)
    loads[2].wait()
    if outer <= 8:
        turn = sorted(range(outer), key=lambda k: [k >> i & 1 for i in range(outer)])
        ahead = min(2, outer - 1)
        for k in turn[1 : ahead + 1]:
            relay(k)
        for i, k in enumerate(turn):
            if 0 < i and i + ahead < outer:
                relay(turn[i + ahead])
            absorb(k, i == 0)
    else:
        absorb(0, True)

        def later(k, c):
            relay(k)
            absorb(k, False)
            return c

        lax.fori_loop(1, outer, later, 0)

    if outer > 1:
        for which in range(2):
            sent = (kz, vz)[which]
            pltpu.make_async_copy(sent, sent, zsend.at[which]).wait()

    def drain(k, c):
        for which in range(2):
            dst = (kd, vd)[which].at[k, others]
            pltpu.make_async_copy(dst, dst, psend.at[k, which]).wait()
        return c

    steps(0, outer, drain)


def finish(acc, total, out_ref):
    block, q_cols = out_ref.shape
    for g in range(q_cols // HD):
        lane = slice(g * block, (g + 1) * block)
        part = acc[:, lane] / total[:, lane]
        out_ref[:, g * HD : (g + 1) * HD] = part.T.astype(out_ref.dtype)


def local(devices, heads, queries, keys, values, block_order):
    inner = 2 if devices % 2 == 0 else 1
    outer = devices // inner
    rows, cols = keys.shape
    block, q_cols = queries.shape
    width = cols // heads
    assert width == HD and rows * heads == block
    bf16, f32 = jnp.bfloat16, jnp.float32
    far = max(outer - 1, 1)
    lanes = q_cols // HD * block
    acc, total = pl.pallas_call(
        functools.partial(kernel, outer, inner, heads),
        out_shape=(
            pltpu.VMEM((HD, lanes), f32),
            pltpu.VMEM((1, lanes), f32),
        ),
        in_specs=[pl.BlockSpec(memory_space=pltpu.SMEM)]
        + [pl.BlockSpec(memory_space=pltpu.HBM)] * 3,
        out_specs=[pl.BlockSpec(memory_space=pltpu.VMEM)] * 2,
        scratch_shapes=[
            pltpu.VMEM((block, q_cols), bf16),
            pltpu.VMEM((rows, cols), bf16),
            pltpu.VMEM((rows, cols), bf16),
            pltpu.VMEM((far, rows, cols), bf16),
            pltpu.VMEM((far, rows, cols), bf16),
            pltpu.VMEM((outer, inner * block, width), bf16),
            pltpu.VMEM((outer, inner * block, width), bf16),
            pltpu.VMEM((1, lanes), f32),
            pltpu.SemaphoreType.DMA((3,)),
            pltpu.SemaphoreType.DMA((outer, 2)),
            pltpu.SemaphoreType.DMA((2,)),
            pltpu.SemaphoreType.DMA((outer, 2)),
            pltpu.SemaphoreType.DMA((outer, 2)),
            pltpu.SemaphoreType.DMA((outer, 2)),
        ],
        compiler_params=pltpu.CompilerParams(
            collective_id=0, has_side_effects=True, vmem_limit_bytes=67043328 - 600 * 1024
        ),
    )(block_order, queries, keys, values)
    return pl.pallas_call(
        finish,
        out_shape=jax.ShapeDtypeStruct((block, q_cols), queries.dtype),
        in_specs=[pl.BlockSpec(memory_space=pltpu.VMEM)] * 2,
        out_specs=pl.BlockSpec(memory_space=pltpu.VMEM),
        compiler_params=pltpu.CompilerParams(vmem_limit_bytes=8 * 1024 * 1024),
    )(acc, total)


def solution(mesh):
    placed = (P("seq", "head"), P(("seq", "head"), None), P(("seq", "head"), None), P())
    return jax.shard_map(
        functools.partial(local, mesh.shape["seq"], mesh.shape["head"]),
        mesh=mesh, in_specs=placed, out_specs=P("seq", "head"), check_vma=False,
    )
```
